32 devices in a mesh: groups: 2 (over x), seq: 16 (over z, y, core).
Axes of the slice: x: 2, y: 2, z: 4, core: 2. Of those that a mesh axis runs over, the one named last changes fastest.
Arguments:
- queries: bfloat16 [4, 2048, 4096], P('groups', 'seq'), parts along dimension 0, may hold values from -120 to 120
- key_states: bfloat16 [4, 2048, 4096], P('groups', 'seq'), parts along dimension 0, may hold values from -4 to 4
- value_states: bfloat16 [4, 2048, 4096], P('groups', 'seq'), parts along dimension 0, may hold values from -6 to 6
- random_blocks: int32 [4, 32, 3], P('groups'), parts along dimension 0, may hold values from 0 to 31
- global_blocks: int32 [4, 2], P('groups'), parts along dimension 0, may hold values from 0 to 31, as said below
Outputs:
- attended: bfloat16 [4, 2048, 4096], P('groups', 'seq'), parts along dimension 0
The draws below stay inside these ranges and needn't reach their ends.
There are 2 independent parts, one for each index of `groups`. The reference program is written for one: setup_inputs(seed, part) draws one part's arguments, and reference() takes and returns one part's arrays. A program takes and returns all parts, laid end to end along the dimension named above; each array names one. Nothing has to cross between parts.
Inputs may be any that keep to these rules, and one draw needn't show every extreme that they name: `global_blocks`: the 2 global blocks of a document are different, the first below 16 and the second not.
All inputs are finite; a program needn't handle non-finite values.
Results may differ from the reference program's by a relative error of at most 0.008.
Values may be sent and summed in bfloat16 or wider, within the bound.
A program may use at most 128 MiB of HBM per device.

```python
import math
import jax
import jax.numpy as jnp
from jax import lax

HEADS = 32
HEAD_DIM = 128
BLOCK = 64
NGLOB = 2
NRAND = 3
DOCS = 2
NBLK = 32
LEN = 2048
ATT = 4096


def drawn_parts(key):
    base = jnp.clip(jax.random.normal(jax.random.fold_in(key, 7), (DOCS, LEN, ATT), jnp.float32), -4.0, 4.0)
    return base


def draw_key_states(key, part):
    base = drawn_parts(key)
    return base.astype(jnp.bfloat16)


def draw_queries(key, part):
    fresh = jnp.clip(jax.random.normal(jax.random.fold_in(key, 5), (DOCS, LEN, ATT), jnp.float32), -4.0, 4.0)
    return fresh.astype(jnp.bfloat16)


def draw_global_blocks(key, part):
    lower = jax.random.randint(jax.random.fold_in(key, 3), (DOCS, 1), 0, NBLK // 2)
    upper = jax.random.randint(jax.random.fold_in(key, 4), (DOCS, 1), NBLK // 2, NBLK)
    documents = jnp.arange(DOCS, dtype=jnp.int32)[:, None]
    high_pick = jax.random.randint(jax.random.fold_in(key, 6), (), 0, DOCS)
    low_pick = jax.random.randint(jax.random.fold_in(key, 8), (), 0, DOCS)
    upper = jnp.where(documents == high_pick, NBLK - 1, upper)
    lower = jnp.where(documents == low_pick, 0, lower)
    return jnp.concatenate([lower, upper], axis=1).astype(jnp.int32)


def touch_ends(values, rng, low, top_value):
    longest = values.shape.index(max(values.shape))
    spots = []
    for shift in (0, 1):
        where = [jax.random.randint(jax.random.fold_in(rng, axis), (), 0, length) for axis, length in enumerate(values.shape)]
        where[longest] = (where[longest] + shift) % values.shape[longest]
        spots.append(tuple(where))
    return values.at[spots[0]].set(low).at[spots[1]].set(top_value)


def block_scale(rng, shape, shards, low, high):
    factor_of, own = 1.0, jax.random.fold_in(rng, 6)
    for dim, parts in shards:
        draws = jnp.exp(jax.random.uniform(jax.random.fold_in(own, dim), (parts,), jnp.float32, low / len(shards), high / len(shards)))
        factor_of = factor_of * jnp.repeat(draws, shape[dim] // parts).reshape([-1 if axis == dim else 1 for axis in range(len(shape))])
    return factor_of


def normal_values(stream_key, shape, deviation, bound, cuts=(), kind=jnp.bfloat16):
    gain = block_scale(stream_key, shape, cuts, -0.22, 0.18) if cuts else 1.0
    drawn = jax.random.normal(stream_key, shape, jnp.float32) * deviation * gain
    return jnp.minimum(jnp.maximum(drawn, -bound), bound).astype(kind)


def setup_inputs(seed: int = 0, part: int = 0) -> dict:
    seeds = jax.random.split(jax.random.key(seed), 6)
    part_keys = jax.random.split(jax.random.fold_in(seeds[5], part), 6)
    return {
        "queries": draw_queries(jax.random.fold_in(jax.random.fold_in(seeds[5], part), 71), part),
        "key_states": draw_key_states(jax.random.fold_in(jax.random.fold_in(seeds[5], part), 71), part),
        "value_states": normal_values(part_keys[2], (DOCS, LEN, ATT), 1.0, 6.0, ((1, 16),)),
        "random_blocks": touch_ends(jax.random.randint(part_keys[3], (DOCS, NBLK, NRAND), 0, NBLK), jax.random.fold_in(part_keys[3], 1), 0, NBLK - 1).astype(jnp.int32),
        "global_blocks": draw_global_blocks(jax.random.fold_in(jax.random.fold_in(seeds[5], part), 71), part),
    }


def soft_weights(scores):
    row_max = jnp.max(scores, axis=-1, keepdims=True)
    exponent = jnp.exp(scores - row_max)
    return (exponent / jnp.sum(exponent, axis=-1, keepdims=True)).astype(jnp.bfloat16)


def global_rows(query_rows, key_tokens, value_tokens):
    scores = jnp.einsum("qhs,khs->hqk", query_rows.astype(jnp.float32), key_tokens.astype(jnp.float32)) * (HEAD_DIM ** -0.5)
    weights = soft_weights(scores)
    return jnp.einsum("hqk,khs->qhs", weights.astype(jnp.float32), value_tokens.astype(jnp.float32)).astype(jnp.bfloat16)


def reference(queries, key_states, value_states, random_blocks, global_blocks):
    results = []
    per_step = math.gcd(NBLK, 8)
    step_count = NBLK // per_step
    for document in range(DOCS):
        query_blocks = queries[document].reshape(NBLK, BLOCK, HEADS, HEAD_DIM)
        key_blocks = key_states[document].reshape(NBLK, BLOCK, HEADS, HEAD_DIM)
        value_blocks = value_states[document].reshape(NBLK, BLOCK, HEADS, HEAD_DIM)
        indices = jnp.arange(NBLK, dtype=jnp.int32)
        globals_here = global_blocks[document].astype(jnp.int32)
        listed = jnp.concatenate([jnp.broadcast_to(globals_here[None, :], (NBLK, NGLOB)), (indices - 1)[:, None], indices[:, None], (indices + 1)[:, None], random_blocks[document].astype(jnp.int32)], axis=1)
        live_mask = jnp.concatenate([jnp.ones((NBLK, NGLOB), jnp.bool_), (indices >= 1)[:, None], jnp.ones((NBLK, 1), jnp.bool_), (indices + 1 < NBLK)[:, None], jnp.ones((NBLK, NRAND), jnp.bool_)], axis=1)
        listed = jnp.clip(listed, 0, NBLK - 1).astype(jnp.int32)

        def one_group(packed):
            query_group, listed_group, live_group = packed
            gathered_keys = jnp.take(key_blocks, listed_group, axis=0).reshape(per_step, -1, HEADS, HEAD_DIM)
            gathered_values = jnp.take(value_blocks, listed_group, axis=0).reshape(per_step, -1, HEADS, HEAD_DIM)
            scores = jnp.einsum("pqhs,pkhs->phqk", query_group.astype(jnp.float32), gathered_keys.astype(jnp.float32)) * (HEAD_DIM ** -0.5)
            live_tokens = jnp.repeat(live_group, BLOCK, axis=1)
            scores = jnp.where(live_tokens[:, None, None, :], scores, -1e30)
            weights = soft_weights(scores)
            return jnp.einsum("phqk,pkhs->pqhs", weights.astype(jnp.float32), gathered_values.astype(jnp.float32)).astype(jnp.bfloat16)

        local = lax.map(one_group, (query_blocks.reshape(step_count, per_step, BLOCK, HEADS, HEAD_DIM), listed.reshape(step_count, per_step, -1), live_mask.reshape(step_count, per_step, -1)))
        local = local.reshape(NBLK, BLOCK, HEADS, HEAD_DIM)
        key_tokens = key_states[document].reshape(LEN, HEADS, HEAD_DIM)
        value_tokens = value_states[document].reshape(LEN, HEADS, HEAD_DIM)
        for slot_index in range(NGLOB):
            where_block = globals_here[slot_index]
            rows_here = lax.dynamic_index_in_dim(query_blocks, where_block, 0, keepdims=False)
            local = lax.dynamic_update_index_in_dim(local, global_rows(rows_here, key_tokens, value_tokens), where_block, 0)
        results.append(local.reshape(LEN, ATT))
    return jnp.stack(results)
```

```python
import functools
import math

import jax
import jax.numpy as jnp
from jax import lax
from jax.experimental import pallas as pl
from jax.experimental.pallas import tpu as pltpu
from jax.sharding import PartitionSpec as P

HEAD_DIM = 128
BLOCK = 64
NGLOB = 2
NRAND = 3


def from_partner(block, axis, distance):
    count = lax.axis_size(axis)
    route = []
    for low in range(count):
        high = low | 1 << distance
        if high != low and high < count:
            route += [(low, high), (high, low)]
    return lax.ppermute(block, axis, route)


def attend_kernel(total_blocks, listed, info, q_ref, ko_ref, kt_ref, vo_ref, vt_ref, o_ref, k_all, v_all):
    rows = q_ref.shape[0]
    count = rows // BLOCK
    width = NGLOB + 3 + NRAND
    scale = HEAD_DIM ** (-0.5)
    k_all[pl.ds(0, rows), :] = ko_ref[...]
    k_all[pl.ds(rows, rows), :] = kt_ref[...]
    v_all[pl.ds(0, rows), :] = vo_ref[...]
    v_all[pl.ds(rows, rows), :] = vt_ref[...]
    parity = info[0]
    per_step = math.gcd(count, 4)
    column = lax.broadcasted_iota(jnp.int32, (BLOCK, width * BLOCK), 1) // BLOCK
    contract = (((1,), (1,)), ((), ()))

    def gather(ref, place):
        parts = []
        for slot in range(width):
            at = pl.multiple_of(listed[place * width + slot] * BLOCK, BLOCK)
            parts.append(ref[pl.ds(at, BLOCK), :])
        return jnp.concatenate(parts, axis=0)

    def step(index, carry):
        places = [index * per_step + sub for sub in range(per_step)]
        scores = []
        for place in places:
            query = q_ref[pl.ds(pl.multiple_of(place * BLOCK, BLOCK), BLOCK), :]
            score = lax.dot_general(query, gather(k_all, place), contract, preferred_element_type=jnp.float32)
            position = 2 * place + parity
            dead = jnp.where(position == 0, NGLOB, jnp.where(position == total_blocks - 1, NGLOB + 2, -1))
            scores.append(jnp.where(column == dead, -1e30, score))
        results = []
        for place, score in zip(places, scores):
            exponent = jnp.exp((score - jnp.max(score, axis=1, keepdims=True)) * scale)
            total = jnp.sum(exponent, axis=1, keepdims=True)
            weights = exponent.astype(jnp.bfloat16)
            summed = jnp.dot(weights, gather(v_all, place), preferred_element_type=jnp.float32)
            results.append((summed / total).astype(jnp.bfloat16))
        for place, result in zip(places, results):
            o_ref[pl.ds(pl.multiple_of(place * BLOCK, BLOCK), BLOCK), :] = result
        return carry

    lax.fori_loop(0, count // per_step, step, 0)
    chunk = math.gcd(2 * rows, 1024)
    for slot in range(NGLOB):
        block = info[1 + slot]

        @pl.when(block % 2 == parity)
        def _():
            at = pl.multiple_of((block // 2) * BLOCK, BLOCK)
            query = q_ref[pl.ds(at, BLOCK), :]

            def part(index, carry):
                top, total, summed = carry
                here = pl.ds(pl.multiple_of(index * chunk, chunk), chunk)
                score = lax.dot_general(query, k_all[here, :], contract, preferred_element_type=jnp.float32)
                new_top = jnp.maximum(top, jnp.max(score, axis=1, keepdims=True))
                shrink = jnp.exp((top - new_top) * scale)
                exponent = jnp.exp((score - new_top) * scale)
                total = total * shrink + jnp.sum(exponent, axis=1, keepdims=True)
                summed = summed * shrink + jnp.dot(
                    exponent.astype(jnp.bfloat16), v_all[here, :], preferred_element_type=jnp.float32
                )
                return new_top, total, summed

            start = (
                jnp.full((BLOCK, 1), -1e30, jnp.float32),
                jnp.zeros((BLOCK, 1), jnp.float32),
                jnp.zeros((BLOCK, HEAD_DIM), jnp.float32),
            )
            _, total, summed = lax.fori_loop(0, 2 * rows // chunk, part, start)
            o_ref[pl.ds(at, BLOCK), :] = (summed / total).astype(jnp.bfloat16)


def per_device(queries, key_states, value_states, random_blocks, global_blocks):
    devices = lax.axis_size("seq")
    device = lax.axis_index("seq")
    documents = queries.shape[0]
    head_groups = devices // (2 * documents)
    group_width = queries.shape[2] // head_groups
    heads_here = group_width // HEAD_DIM
    block_len = BLOCK
    total_blocks = 2 * devices
    parity = device % 2
    document = device // (2 * head_groups)

    def by_parity(states):
        pieces = states.reshape(documents, 2, block_len, head_groups, group_width)
        return pieces.transpose(0, 3, 1, 2, 4).reshape(devices, block_len, group_width)

    query_recv, key_half, value_half = (
        lax.all_to_all(by_parity(queries), "seq", split_axis=0, concat_axis=1, tiled=True),
        lax.all_to_all(by_parity(key_states), "seq", split_axis=0, concat_axis=1, tiled=True),
        lax.all_to_all(by_parity(value_states), "seq", split_axis=0, concat_axis=1, tiled=True),
    )
    key_other, value_other = from_partner((key_half, value_half), "seq", 0)

    document_lists = lax.dynamic_index_in_dim(random_blocks, document, 0, keepdims=False)
    own_lists = lax.dynamic_index_in_dim(
        document_lists.reshape(devices, 2, NRAND), parity, 1, keepdims=False
    )
    globals_here = lax.dynamic_index_in_dim(global_blocks, document, 0, keepdims=False)
    positions = 2 * jnp.arange(devices, dtype=jnp.int32) + parity
    listed = jnp.concatenate(
        [
            jnp.broadcast_to(globals_here[None, :], (devices, NGLOB)),
            (positions - 1)[:, None],
            positions[:, None],
            (positions + 1)[:, None],
            own_lists,
        ],
        axis=1,
    )
    listed = jnp.clip(listed, 0, total_blocks - 1)
    listed = listed // 2 + jnp.where(listed % 2 == parity, 0, devices)
    info = jnp.concatenate([jnp.reshape(parity, (1,)), globals_here]).astype(jnp.int32)
    rows = devices * block_len
    column_block = pl.BlockSpec((rows, HEAD_DIM), lambda head, *_: (0, head))
    attended = pl.pallas_call(
        functools.partial(attend_kernel, total_blocks),
        out_shape=jax.ShapeDtypeStruct((rows, group_width), jnp.bfloat16),
        grid_spec=pltpu.PrefetchScalarGridSpec(
            num_scalar_prefetch=2,
            grid=(heads_here,),
            in_specs=[column_block] * 5,
            out_specs=column_block,
            scratch_shapes=[pltpu.VMEM((2 * rows, HEAD_DIM), jnp.bfloat16)] * 2,
        ),
    )(
        listed.reshape(-1).astype(jnp.int32),
        info,
        query_recv.reshape(rows, group_width),
        key_half.reshape(rows, group_width),
        key_other.reshape(rows, group_width),
        value_half.reshape(rows, group_width),
        value_other.reshape(rows, group_width),
    )
    returned = lax.all_to_all(
        attended.reshape(devices, block_len, group_width),
        "seq",
        split_axis=0,
        concat_axis=0,
        tiled=True,
    )
    returned = returned.reshape(documents, head_groups, 2, block_len, group_width).transpose(
        0, 2, 3, 1, 4
    )
    return returned.reshape(documents, 2 * block_len, head_groups * group_width)


def solution(mesh):
    placed = (
        P("groups", "seq", None),
        P("groups", "seq", None),
        P("groups", "seq", None),
        P("groups", None, None),
        P("groups", None),
    )
    return jax.shard_map(
        per_device, mesh=mesh, in_specs=placed, out_specs=P("groups", "seq", None), check_vma=False
    )
```

```python
import functools
import math

import jax
import jax.numpy as jnp
from jax import lax
from jax.experimental import pallas as pl
from jax.experimental.pallas import tpu as pltpu
from jax.sharding import PartitionSpec as P

HEAD_DIM = 128
BLOCK = 64
NGLOB = 2
NRAND = 3


def from_partner(block, axis, distance):
    count = lax.axis_size(axis)
    route = []
    for low in range(count):
        high = low | 1 << distance
        if high != low and high < count:
            route += [(low, high), (high, low)]
    return lax.ppermute(block, axis, route)


def attend_kernel(total_blocks, listed, info, q_ref, ko_ref, kt_ref, vo_ref, vt_ref, o_ref, k_all, v_all):
    rows = q_ref.shape[0]
    count = rows // BLOCK
    width = NGLOB + 3 + NRAND
    scale = HEAD_DIM ** (-0.5)
    k_all[pl.ds(0, rows), :] = ko_ref[...]
    k_all[pl.ds(rows, rows), :] = kt_ref[...]
    v_all[pl.ds(0, rows), :] = vo_ref[...]
    v_all[pl.ds(rows, rows), :] = vt_ref[...]
    parity = info[0]
    per_step = math.gcd(count, 4)
    column = lax.broadcasted_iota(jnp.int32, (BLOCK, width * BLOCK), 1) // BLOCK
    contract = (((1,), (1,)), ((), ()))

    def gather(ref, place):
        parts = []
        for slot in range(width):
            at = pl.multiple_of(listed[place * width + slot] * BLOCK, BLOCK)
            parts.append(ref[pl.ds(at, BLOCK), :])
        return jnp.concatenate(parts, axis=0)

    def step(index, carry):
        places = [index * per_step + sub for sub in range(per_step)]
        scores = []
        for place in places:
            query = q_ref[pl.ds(pl.multiple_of(place * BLOCK, BLOCK), BLOCK), :]
            score = lax.dot_general(query, gather(k_all, place), contract, preferred_element_type=jnp.float32)
            position = 2 * place + parity
            dead = jnp.where(position == 0, NGLOB, jnp.where(position == total_blocks - 1, NGLOB + 2, -1))
            scores.append(jnp.where(column == dead, -1e30, score))
        results = []
        for place, score in zip(places, scores):
            exponent = jnp.exp((score - jnp.max(score, axis=1, keepdims=True)) * scale)
            total = jnp.sum(exponent, axis=1, keepdims=True)
            weights = exponent.astype(jnp.bfloat16)
            summed = jnp.dot(weights, gather(v_all, place), preferred_element_type=jnp.float32)
            results.append((summed / total).astype(jnp.bfloat16))
        for place, result in zip(places, results):
            o_ref[pl.ds(pl.multiple_of(place * BLOCK, BLOCK), BLOCK), :] = result
        return carry

    lax.fori_loop(0, count // per_step, step, 0)
    chunk = math.gcd(2 * rows, 1024)
    for slot in range(NGLOB):
        block = info[1 + slot]

        @pl.when(block % 2 == parity)
        def _():
            at = pl.multiple_of((block // 2) * BLOCK, BLOCK)
            query = q_ref[pl.ds(at, BLOCK), :]

            def part(index, carry):
                top, total, summed = carry
                here = pl.ds(pl.multiple_of(index * chunk, chunk), chunk)
                score = lax.dot_general(query, k_all[here, :], contract, preferred_element_type=jnp.float32)
                new_top = jnp.maximum(top, jnp.max(score, axis=1, keepdims=True))
                shrink = jnp.exp((top - new_top) * scale)
                exponent = jnp.exp((score - new_top) * scale)
                total = total * shrink + jnp.sum(exponent, axis=1, keepdims=True)
                summed = summed * shrink + jnp.dot(
                    exponent.astype(jnp.bfloat16), v_all[here, :], preferred_element_type=jnp.float32
                )
                return new_top, total, summed

            start = (
                jnp.full((BLOCK, 1), -1e30, jnp.float32),
                jnp.zeros((BLOCK, 1), jnp.float32),
                jnp.zeros((BLOCK, HEAD_DIM), jnp.float32),
            )
            _, total, summed = lax.fori_loop(0, 2 * rows // chunk, part, start)
            o_ref[pl.ds(at, BLOCK), :] = (summed / total).astype(jnp.bfloat16)


def fused_kernel(
    documents, chunk_count, listed, info, chosen, q_hbm, k_hbm, v_hbm, out_hbm, *scratch
):
    landed, made = scratch[:chunk_count], scratch[chunk_count : 2 * chunk_count]
    send_sem, recv_sem, back_send_sem, back_recv_sem = scratch[2 * chunk_count :]
    devices = lax.axis_size("seq")
    me = lax.axis_index("seq")
    head_groups = devices // documents
    held_blocks = q_hbm.shape[1]
    count = devices * held_blocks
    chunk_width = landed[0].shape[3]
    group_width = chunk_width * chunk_count
    width = NGLOB + 3 + NRAND
    scale = HEAD_DIM ** (-0.5)
    sources = (k_hbm, v_hbm, q_hbm)

    def outward(target, chunk):
        column = pl.multiple_of(lax.rem(target, head_groups) * group_width + chunk * chunk_width, HEAD_DIM)
        return lax.div(target, head_groups), pl.ds(column, chunk_width)

    def blocks_of(device):
        return pl.ds(device * held_blocks, held_blocks)

    barrier = pltpu.get_barrier_semaphore()

    def greet(step, carry):
        pl.semaphore_signal(
            barrier, inc=1, device_id={"seq": lax.rem(me + step, devices)}, device_id_type=pl.DeviceIdType.MESH
        )
        return carry

    lax.fori_loop(1, devices, greet, 0)
    pl.semaphore_wait(barrier, devices - 1)

    for chunk in range(chunk_count):

        def send(step, carry):
            target = lax.rem(me + step, devices)
            document, columns = outward(target, chunk)
            for which, source in enumerate(sources):
                pltpu.make_async_remote_copy(
                    src_ref=source.at[document, :, :, columns],
                    dst_ref=landed[chunk].at[which, blocks_of(me)],
                    send_sem=send_sem.at[chunk],
                    recv_sem=recv_sem.at[chunk],
                    device_id={"seq": target},
                    device_id_type=pl.DeviceIdType.MESH,
                ).start()
            return carry

        lax.fori_loop(1, devices, send, 0)
        document, columns = outward(me, chunk)
        for which, source in enumerate(sources):
            pltpu.make_async_copy(
                source.at[document, :, :, columns], landed[chunk].at[which, blocks_of(me)], recv_sem.at[chunk]
            ).start()

    per_step = math.gcd(count, 4)
    column_block = lax.broadcasted_iota(jnp.int32, (BLOCK, width * BLOCK), 1) // BLOCK
    contract = (((1,), (1,)), ((), ()))
    long_chunk = math.gcd(count, 16)

    def attend(held, result_ref, head):
        lanes = slice(head * HEAD_DIM, (head + 1) * HEAD_DIM)

        def gather(which, place):
            parts = []
            for slot in range(width):
                parts.append(held[which, listed[place * width + slot], :, lanes])
            return jnp.concatenate(parts, axis=0)

        global_results = []
        for slot in range(NGLOB):
            query = held[2, info[slot], :, lanes]
            top = jnp.full((BLOCK, 1), -1e30, jnp.float32)
            total = jnp.zeros((BLOCK, 1), jnp.float32)
            summed = jnp.zeros((BLOCK, HEAD_DIM), jnp.float32)
            for start in range(0, count, long_chunk):
                here = slice(start, start + long_chunk)
                score = lax.dot_general(query, held[0, here, :, lanes].reshape(-1, HEAD_DIM), contract, preferred_element_type=jnp.float32)
                new_top = jnp.maximum(top, jnp.max(score, axis=1, keepdims=True))
                shrink = jnp.exp((top - new_top) * scale)
                exponent = jnp.exp((score - new_top) * scale)
                total = total * shrink + jnp.sum(exponent, axis=1, keepdims=True)
                summed = summed * shrink + jnp.dot(
                    exponent.astype(jnp.bfloat16), held[1, here, :, lanes].reshape(-1, HEAD_DIM), preferred_element_type=jnp.float32
                )
                top = new_top
            global_results.append(summed / total)

        def step(index, carry):
            places = [index * per_step + sub for sub in range(per_step)]
            scores = []
            for place in places:
                query = held[2, place, :, lanes]
                score = lax.dot_general(query, gather(0, place), contract, preferred_element_type=jnp.float32)
                dead = jnp.where(place == 0, NGLOB, jnp.where(place == count - 1, NGLOB + 2, -1))
                scores.append(jnp.where(column_block == dead, -1e30, score))
            results = []
            for place, score in zip(places, scores):
                exponent = jnp.exp((score - jnp.max(score, axis=1, keepdims=True)) * scale)
                total = jnp.sum(exponent, axis=1, keepdims=True)
                summed = jnp.dot(exponent.astype(jnp.bfloat16), gather(1, place), preferred_element_type=jnp.float32)
                result = summed / total
                result = result * chosen[place * (NGLOB + 1) + NGLOB]
                for slot in range(NGLOB):
                    result += global_results[slot] * chosen[place * (NGLOB + 1) + slot]
                results.append(result.astype(jnp.bfloat16))
            for place, result in zip(places, results):
                result_ref[place, :, lanes] = result
            return carry

        lax.fori_loop(0, count // per_step, step, 0)

    def give_back(chunk):
        document, columns = outward(me, chunk)

        def send(step, carry):
            target = lax.rem(me + step, devices)
            pltpu.make_async_remote_copy(
                src_ref=made[chunk].at[blocks_of(target)],
                dst_ref=out_hbm.at[document, :, :, columns],
                send_sem=back_send_sem.at[chunk],
                recv_sem=back_recv_sem,
                device_id={"seq": target},
                device_id_type=pl.DeviceIdType.MESH,
            ).start()
            return carry

        lax.fori_loop(1, devices, send, 0)
        pltpu.make_async_copy(made[chunk].at[blocks_of(me)], out_hbm.at[document, :, :, columns], back_recv_sem).start()

    for chunk in range(chunk_count):
        pltpu.make_async_copy(landed[chunk], landed[chunk], recv_sem.at[chunk]).wait()
        for head in range(chunk_width // HEAD_DIM):
            attend(landed[chunk], made[chunk], head)
        give_back(chunk)
    others = pl.ds(0, count - held_blocks)
    for chunk in range(chunk_count):
        sent = landed[chunk].at[:, others]
        pltpu.make_async_copy(sent, sent, send_sem.at[chunk]).wait()
        sent = made[chunk].at[others]
        pltpu.make_async_copy(sent, sent, back_send_sem.at[chunk]).wait()
    pltpu.make_async_copy(out_hbm, out_hbm, back_recv_sem).wait()


CHUNK_HEADS = 1


def per_device_fused(queries, key_states, value_states, random_blocks, global_blocks):
    devices = lax.axis_size("seq")
    documents, tokens, features = queries.shape
    head_groups = devices // documents
    group_width = features // head_groups
    chunk_width = CHUNK_HEADS * HEAD_DIM
    chunk_count = group_width // chunk_width
    rows = devices * tokens
    total_blocks = rows // BLOCK
    document = lax.axis_index("seq") // head_groups
    own_lists = lax.dynamic_index_in_dim(random_blocks, document, 0, keepdims=False)
    globals_here = lax.dynamic_index_in_dim(global_blocks, document, 0, keepdims=False)
    positions = jnp.arange(total_blocks, dtype=jnp.int32)[:, None]
    listed = jnp.concatenate(
        [
            jnp.broadcast_to(globals_here[None, :], (total_blocks, NGLOB)),
            positions - 1,
            positions,
            positions + 1,
            own_lists,
        ],
        axis=1,
    )
    listed = jnp.clip(listed, 0, total_blocks - 1)
    chosen = (positions == globals_here[None, :]).astype(jnp.float32)
    chosen = jnp.concatenate([chosen, 1.0 - jnp.sum(chosen, axis=1, keepdims=True)], axis=1)
    blocked = (documents, tokens // BLOCK, BLOCK, features)
    returned = pl.pallas_call(
        functools.partial(fused_kernel, documents, chunk_count),
        out_shape=jax.ShapeDtypeStruct(blocked, jnp.bfloat16),
        in_specs=[pl.BlockSpec(memory_space=pltpu.SMEM)] * 3 + [pl.BlockSpec(memory_space=pl.ANY)] * 3,
        out_specs=pl.BlockSpec(memory_space=pl.ANY),
        scratch_shapes=[pltpu.VMEM((3, total_blocks, BLOCK, chunk_width), jnp.bfloat16)] * chunk_count
        + [pltpu.VMEM((total_blocks, BLOCK, chunk_width), jnp.bfloat16)] * chunk_count
        + [
            pltpu.SemaphoreType.DMA((chunk_count,)),
            pltpu.SemaphoreType.DMA((chunk_count,)),
            pltpu.SemaphoreType.DMA((chunk_count,)),
            pltpu.SemaphoreType.DMA,
        ],
        compiler_params=pltpu.CompilerParams(collective_id=0, has_side_effects=True),
    )(
        listed.reshape(-1).astype(jnp.int32),
        globals_here.astype(jnp.int32),
        chosen.reshape(-1),
        queries.reshape(blocked),
        key_states.reshape(blocked),
        value_states.reshape(blocked),
    )
    return returned.reshape(queries.shape)


def per_device(queries, key_states, value_states, random_blocks, global_blocks):
    devices = lax.axis_size("seq")
    device = lax.axis_index("seq")
    documents = queries.shape[0]
    head_groups = devices // (2 * documents)
    group_width = queries.shape[2] // head_groups
    heads_here = group_width // HEAD_DIM
    block_len = BLOCK
    total_blocks = 2 * devices
    parity = device % 2
    document = device // (2 * head_groups)

    def by_parity(states):
        pieces = states.reshape(documents, 2, block_len, head_groups, group_width)
        return pieces.transpose(0, 3, 1, 2, 4).reshape(devices, block_len, group_width)

    query_recv, key_half, value_half = (
        lax.all_to_all(by_parity(queries), "seq", split_axis=0, concat_axis=1, tiled=True),
        lax.all_to_all(by_parity(key_states), "seq", split_axis=0, concat_axis=1, tiled=True),
        lax.all_to_all(by_parity(value_states), "seq", split_axis=0, concat_axis=1, tiled=True),
    )
    key_other, value_other = from_partner((key_half, value_half), "seq", 0)

    document_lists = lax.dynamic_index_in_dim(random_blocks, document, 0, keepdims=False)
    own_lists = lax.dynamic_index_in_dim(
        document_lists.reshape(devices, 2, NRAND), parity, 1, keepdims=False
    )
    globals_here = lax.dynamic_index_in_dim(global_blocks, document, 0, keepdims=False)
    positions = 2 * jnp.arange(devices, dtype=jnp.int32) + parity
    listed = jnp.concatenate(
        [
            jnp.broadcast_to(globals_here[None, :], (devices, NGLOB)),
            (positions - 1)[:, None],
            positions[:, None],
            (positions + 1)[:, None],
            own_lists,
        ],
        axis=1,
    )
    listed = jnp.clip(listed, 0, total_blocks - 1)
    listed = listed // 2 + jnp.where(listed % 2 == parity, 0, devices)
    info = jnp.concatenate([jnp.reshape(parity, (1,)), globals_here]).astype(jnp.int32)
    rows = devices * block_len
    column_block = pl.BlockSpec((rows, HEAD_DIM), lambda head, *_: (0, head))
    attended = pl.pallas_call(
        functools.partial(attend_kernel, total_blocks),
        out_shape=jax.ShapeDtypeStruct((rows, group_width), jnp.bfloat16),
        grid_spec=pltpu.PrefetchScalarGridSpec(
            num_scalar_prefetch=2,
            grid=(heads_here,),
            in_specs=[column_block] * 5,
            out_specs=column_block,
            scratch_shapes=[pltpu.VMEM((2 * rows, HEAD_DIM), jnp.bfloat16)] * 2,
        ),
    )(
        listed.reshape(-1).astype(jnp.int32),
        info,
        query_recv.reshape(rows, group_width),
        key_half.reshape(rows, group_width),
        key_other.reshape(rows, group_width),
        value_half.reshape(rows, group_width),
        value_other.reshape(rows, group_width),
    )
    returned = lax.all_to_all(
        attended.reshape(devices, block_len, group_width),
        "seq",
        split_axis=0,
        concat_axis=0,
        tiled=True,
    )
    returned = returned.reshape(documents, head_groups, 2, block_len, group_width).transpose(
        0, 2, 3, 1, 4
    )
    return returned.reshape(documents, 2 * block_len, head_groups * group_width)


def solution(mesh):
    placed = (
        P("groups", "seq", None),
        P("groups", "seq", None),
        P("groups", "seq", None),
        P("groups", None, None),
        P("groups", None),
    )

    def body(queries, *others):
        heads = queries.shape[2] // HEAD_DIM
        groups_needed = lax.axis_size("seq") // queries.shape[0]
        if heads % (groups_needed * CHUNK_HEADS) == 0:
            return per_device_fused(queries, *others)
        return per_device(queries, *others)

    return jax.shard_map(
        body, mesh=mesh, in_specs=placed, out_specs=P("groups", "seq", None), check_vma=False
    )
```

```python
import functools
import math

import jax
import jax.numpy as jnp
from jax import lax
from jax.experimental import pallas as pl
from jax.experimental.pallas import tpu as pltpu
from jax.sharding import PartitionSpec as P

HEAD_DIM = 128
BLOCK = 64
NGLOB = 2
NRAND = 3


def from_partner(block, axis, distance):
    count = lax.axis_size(axis)
    route = []
    for low in range(count):
        high = low | 1 << distance
        if high != low and high < count:
            route += [(low, high), (high, low)]
    return lax.ppermute(block, axis, route)


def attend_kernel(total_blocks, listed, info, q_ref, ko_ref, kt_ref, vo_ref, vt_ref, o_ref, k_all, v_all):
    rows = q_ref.shape[0]
    count = rows // BLOCK
    width = NGLOB + 3 + NRAND
    scale = HEAD_DIM ** (-0.5)
    k_all[pl.ds(0, rows), :] = ko_ref[...]
    k_all[pl.ds(rows, rows), :] = kt_ref[...]
    v_all[pl.ds(0, rows), :] = vo_ref[...]
    v_all[pl.ds(rows, rows), :] = vt_ref[...]
    parity = info[0]
    per_step = math.gcd(count, 4)
    column = lax.broadcasted_iota(jnp.int32, (BLOCK, width * BLOCK), 1) // BLOCK
    contract = (((1,), (1,)), ((), ()))

    def gather(ref, place):
        parts = []
        for slot in range(width):
            at = pl.multiple_of(listed[place * width + slot] * BLOCK, BLOCK)
            parts.append(ref[pl.ds(at, BLOCK), :])
        return jnp.concatenate(parts, axis=0)

    def step(index, carry):
        places = [index * per_step + sub for sub in range(per_step)]
        scores = []
        for place in places:
            query = q_ref[pl.ds(pl.multiple_of(place * BLOCK, BLOCK), BLOCK), :]
            score = lax.dot_general(query, gather(k_all, place), contract, preferred_element_type=jnp.float32)
            position = 2 * place + parity
            dead = jnp.where(position == 0, NGLOB, jnp.where(position == total_blocks - 1, NGLOB + 2, -1))
            scores.append(jnp.where(column == dead, -1e30, score))
        results = []
        for place, score in zip(places, scores):
            exponent = jnp.exp((score - jnp.max(score, axis=1, keepdims=True)) * scale)
            total = jnp.sum(exponent, axis=1, keepdims=True)
            weights = exponent.astype(jnp.bfloat16)
            summed = jnp.dot(weights, gather(v_all, place), preferred_element_type=jnp.float32)
            results.append((summed / total).astype(jnp.bfloat16))
        for place, result in zip(places, results):
            o_ref[pl.ds(pl.multiple_of(place * BLOCK, BLOCK), BLOCK), :] = result
        return carry

    lax.fori_loop(0, count // per_step, step, 0)
    chunk = math.gcd(2 * rows, 1024)
    for slot in range(NGLOB):
        block = info[1 + slot]

        @pl.when(block % 2 == parity)
        def _():
            at = pl.multiple_of((block // 2) * BLOCK, BLOCK)
            query = q_ref[pl.ds(at, BLOCK), :]

            def part(index, carry):
                top, total, summed = carry
                here = pl.ds(pl.multiple_of(index * chunk, chunk), chunk)
                score = lax.dot_general(query, k_all[here, :], contract, preferred_element_type=jnp.float32)
                new_top = jnp.maximum(top, jnp.max(score, axis=1, keepdims=True))
                shrink = jnp.exp((top - new_top) * scale)
                exponent = jnp.exp((score - new_top) * scale)
                total = total * shrink + jnp.sum(exponent, axis=1, keepdims=True)
                summed = summed * shrink + jnp.dot(
                    exponent.astype(jnp.bfloat16), v_all[here, :], preferred_element_type=jnp.float32
                )
                return new_top, total, summed

            start = (
                jnp.full((BLOCK, 1), -1e30, jnp.float32),
                jnp.zeros((BLOCK, 1), jnp.float32),
                jnp.zeros((BLOCK, HEAD_DIM), jnp.float32),
            )
            _, total, summed = lax.fori_loop(0, 2 * rows // chunk, part, start)
            o_ref[pl.ds(at, BLOCK), :] = (summed / total).astype(jnp.bfloat16)


def fused_kernel(
    documents, chunk_count, listed, info, chosen, q_hbm, k_hbm, v_hbm, out_hbm, *scratch
):
    landed, made = scratch[:chunk_count], scratch[chunk_count : 2 * chunk_count]
    send_sem, recv_sem, back_send_sem, back_recv_sem = scratch[2 * chunk_count :]
    devices = lax.axis_size("seq")
    me = lax.axis_index("seq")
    head_groups = devices // documents
    held_blocks = q_hbm.shape[1]
    count = devices * held_blocks
    chunk_width = landed[0].shape[3]
    group_width = chunk_width * chunk_count
    width = NGLOB + 3 + NRAND
    scale = HEAD_DIM ** (-0.5)
    sources = (k_hbm, v_hbm, q_hbm)

    def outward(target, chunk):
        column = pl.multiple_of(lax.rem(target, head_groups) * group_width + chunk * chunk_width, HEAD_DIM)
        return lax.div(target, head_groups), pl.ds(column, chunk_width)

    def blocks_of(device):
        return pl.ds(device * held_blocks, held_blocks)

    barrier = pltpu.get_barrier_semaphore()

    def greet(step, carry):
        pl.semaphore_signal(
            barrier, inc=1, device_id={"seq": lax.rem(me + step, devices)}, device_id_type=pl.DeviceIdType.MESH
        )
        return carry

    lax.fori_loop(1, devices, greet, 0)
    pl.semaphore_wait(barrier, devices - 1)

    half = devices // 2
    side, seat = lax.div(me, half), lax.rem(me, half)

    def far(step):
        return (1 - side) * half + lax.rem(seat + step, half)

    def near(step):
        return side * half + lax.rem(seat + step, half)

    for chunk in range(chunk_count):

        def send(place, step, carry):
            target = place(step)
            document, columns = outward(target, chunk)
            for which, source in enumerate(sources):
                pltpu.make_async_remote_copy(
                    src_ref=source.at[document, :, :, columns],
                    dst_ref=landed[chunk].at[which, blocks_of(me)],
                    send_sem=send_sem.at[chunk],
                    recv_sem=recv_sem.at[chunk],
                    device_id={"seq": target},
                    device_id_type=pl.DeviceIdType.MESH,
                ).start()
            return carry

        lax.fori_loop(0, half, functools.partial(send, far), 0)
        lax.fori_loop(1, half, functools.partial(send, near), 0)
        document, columns = outward(me, chunk)
        for which, source in enumerate(sources):
            pltpu.make_async_copy(
                source.at[document, :, :, columns], landed[chunk].at[which, blocks_of(me)], recv_sem.at[chunk]
            ).start()

    per_step = math.gcd(count, 4)
    column_block = lax.broadcasted_iota(jnp.int32, (BLOCK, width * BLOCK), 1) // BLOCK
    contract = (((1,), (1,)), ((), ()))
    long_chunk = math.gcd(count, 16)

    def attend(held, result_ref, head):
        lanes = slice(head * HEAD_DIM, (head + 1) * HEAD_DIM)

        def gather(which, place):
            parts = []
            for slot in range(width):
                parts.append(held[which, listed[place * width + slot], :, lanes])
            return jnp.concatenate(parts, axis=0)

        global_results = []
        for slot in range(NGLOB):
            query = held[2, info[slot], :, lanes]
            top = jnp.full((BLOCK, 1), -1e30, jnp.float32)
            total = jnp.zeros((BLOCK, 1), jnp.float32)
            summed = jnp.zeros((BLOCK, HEAD_DIM), jnp.float32)
            for start in range(0, count, long_chunk):
                here = slice(start, start + long_chunk)
                score = lax.dot_general(query, held[0, here, :, lanes].reshape(-1, HEAD_DIM), contract, preferred_element_type=jnp.float32)
                new_top = jnp.maximum(top, jnp.max(score, axis=1, keepdims=True))
                shrink = jnp.exp((top - new_top) * scale)
                exponent = jnp.exp((score - new_top) * scale)
                total = total * shrink + jnp.sum(exponent, axis=1, keepdims=True)
                summed = summed * shrink + jnp.dot(
                    exponent.astype(jnp.bfloat16), held[1, here, :, lanes].reshape(-1, HEAD_DIM), preferred_element_type=jnp.float32
                )
                top = new_top
            global_results.append(summed / total)

        def step(index, carry):
            places = [index * per_step + sub for sub in range(per_step)]
            scores = []
            for place in places:
                query = held[2, place, :, lanes]
                score = lax.dot_general(query, gather(0, place), contract, preferred_element_type=jnp.float32)
                dead = jnp.where(place == 0, NGLOB, jnp.where(place == count - 1, NGLOB + 2, -1))
                scores.append(jnp.where(column_block == dead, -1e30, score))
            results = []
            for place, score in zip(places, scores):
                exponent = jnp.exp((score - jnp.max(score, axis=1, keepdims=True)) * scale)
                total = jnp.sum(exponent, axis=1, keepdims=True)
                summed = jnp.dot(exponent.astype(jnp.bfloat16), gather(1, place), preferred_element_type=jnp.float32)
                result = summed / total
                result = result * chosen[place * (NGLOB + 1) + NGLOB]
                for slot in range(NGLOB):
                    result += global_results[slot] * chosen[place * (NGLOB + 1) + slot]
                results.append(result.astype(jnp.bfloat16))
            for place, result in zip(places, results):
                result_ref[place, :, lanes] = result
            return carry

        lax.fori_loop(0, count // per_step, step, 0)

    def give_back(chunk):
        document, columns = outward(me, chunk)

        def send(place, step, carry):
            target = place(step)
            pltpu.make_async_remote_copy(
                src_ref=made[chunk].at[blocks_of(target)],
                dst_ref=out_hbm.at[document, :, :, columns],
                send_sem=back_send_sem.at[chunk],
                recv_sem=back_recv_sem,
                device_id={"seq": target},
                device_id_type=pl.DeviceIdType.MESH,
            ).start()
            return carry

        lax.fori_loop(0, half, functools.partial(send, far), 0)
        lax.fori_loop(1, half, functools.partial(send, near), 0)
        pltpu.make_async_copy(made[chunk].at[blocks_of(me)], out_hbm.at[document, :, :, columns], back_recv_sem).start()

    for chunk in range(chunk_count):
        pltpu.make_async_copy(landed[chunk], landed[chunk], recv_sem.at[chunk]).wait()
        for head in range(chunk_width // HEAD_DIM):
            attend(landed[chunk], made[chunk], head)
        give_back(chunk)
    others = pl.ds(0, count - held_blocks)
    for chunk in range(chunk_count):
        sent = landed[chunk].at[:, others]
        pltpu.make_async_copy(sent, sent, send_sem.at[chunk]).wait()
        sent = made[chunk].at[others]
        pltpu.make_async_copy(sent, sent, back_send_sem.at[chunk]).wait()
    pltpu.make_async_copy(out_hbm, out_hbm, back_recv_sem).wait()


CHUNK_HEADS = 1


def per_device_fused(queries, key_states, value_states, random_blocks, global_blocks):
    devices = lax.axis_size("seq")
    documents, tokens, features = queries.shape
    head_groups = devices // documents
    group_width = features // head_groups
    chunk_width = CHUNK_HEADS * HEAD_DIM
    chunk_count = group_width // chunk_width
    rows = devices * tokens
    total_blocks = rows // BLOCK
    document = lax.axis_index("seq") // head_groups
    own_lists = lax.dynamic_index_in_dim(random_blocks, document, 0, keepdims=False)
    globals_here = lax.dynamic_index_in_dim(global_blocks, document, 0, keepdims=False)
    positions = jnp.arange(total_blocks, dtype=jnp.int32)[:, None]
    listed = jnp.concatenate(
        [
            jnp.broadcast_to(globals_here[None, :], (total_blocks, NGLOB)),
            positions - 1,
            positions,
            positions + 1,
            own_lists,
        ],
        axis=1,
    )
    listed = jnp.clip(listed, 0, total_blocks - 1)
    chosen = (positions == globals_here[None, :]).astype(jnp.float32)
    chosen = jnp.concatenate([chosen, 1.0 - jnp.sum(chosen, axis=1, keepdims=True)], axis=1)
    blocked = (documents, tokens // BLOCK, BLOCK, features)
    returned = pl.pallas_call(
        functools.partial(fused_kernel, documents, chunk_count),
        out_shape=jax.ShapeDtypeStruct(blocked, jnp.bfloat16),
        in_specs=[pl.BlockSpec(memory_space=pltpu.SMEM)] * 3 + [pl.BlockSpec(memory_space=pl.ANY)] * 3,
        out_specs=pl.BlockSpec(memory_space=pl.ANY),
        scratch_shapes=[pltpu.VMEM((3, total_blocks, BLOCK, chunk_width), jnp.bfloat16)] * chunk_count
        + [pltpu.VMEM((total_blocks, BLOCK, chunk_width), jnp.bfloat16)] * chunk_count
        + [
            pltpu.SemaphoreType.DMA((chunk_count,)),
            pltpu.SemaphoreType.DMA((chunk_count,)),
            pltpu.SemaphoreType.DMA((chunk_count,)),
            pltpu.SemaphoreType.DMA,
        ],
        compiler_params=pltpu.CompilerParams(collective_id=0, has_side_effects=True),
    )(
        listed.reshape(-1).astype(jnp.int32),
        globals_here.astype(jnp.int32),
        chosen.reshape(-1),
        queries.reshape(blocked),
        key_states.reshape(blocked),
        value_states.reshape(blocked),
    )
    return returned.reshape(queries.shape)


def per_device(queries, key_states, value_states, random_blocks, global_blocks):
    devices = lax.axis_size("seq")
    device = lax.axis_index("seq")
    documents = queries.shape[0]
    head_groups = devices // (2 * documents)
    group_width = queries.shape[2] // head_groups
    heads_here = group_width // HEAD_DIM
    block_len = BLOCK
    total_blocks = 2 * devices
    parity = device % 2
    document = device // (2 * head_groups)

    def by_parity(states):
        pieces = states.reshape(documents, 2, block_len, head_groups, group_width)
        return pieces.transpose(0, 3, 1, 2, 4).reshape(devices, block_len, group_width)

    query_recv, key_half, value_half = (
        lax.all_to_all(by_parity(queries), "seq", split_axis=0, concat_axis=1, tiled=True),
        lax.all_to_all(by_parity(key_states), "seq", split_axis=0, concat_axis=1, tiled=True),
        lax.all_to_all(by_parity(value_states), "seq", split_axis=0, concat_axis=1, tiled=True),
    )
    key_other, value_other = from_partner((key_half, value_half), "seq", 0)

    document_lists = lax.dynamic_index_in_dim(random_blocks, document, 0, keepdims=False)
    own_lists = lax.dynamic_index_in_dim(
        document_lists.reshape(devices, 2, NRAND), parity, 1, keepdims=False
    )
    globals_here = lax.dynamic_index_in_dim(global_blocks, document, 0, keepdims=False)
    positions = 2 * jnp.arange(devices, dtype=jnp.int32) + parity
    listed = jnp.concatenate(
        [
            jnp.broadcast_to(globals_here[None, :], (devices, NGLOB)),
            (positions - 1)[:, None],
            positions[:, None],
            (positions + 1)[:, None],
            own_lists,
        ],
        axis=1,
    )
    listed = jnp.clip(listed, 0, total_blocks - 1)
    listed = listed // 2 + jnp.where(listed % 2 == parity, 0, devices)
    info = jnp.concatenate([jnp.reshape(parity, (1,)), globals_here]).astype(jnp.int32)
    rows = devices * block_len
    column_block = pl.BlockSpec((rows, HEAD_DIM), lambda head, *_: (0, head))
    attended = pl.pallas_call(
        functools.partial(attend_kernel, total_blocks),
        out_shape=jax.ShapeDtypeStruct((rows, group_width), jnp.bfloat16),
        grid_spec=pltpu.PrefetchScalarGridSpec(
            num_scalar_prefetch=2,
            grid=(heads_here,),
            in_specs=[column_block] * 5,
            out_specs=column_block,
            scratch_shapes=[pltpu.VMEM((2 * rows, HEAD_DIM), jnp.bfloat16)] * 2,
        ),
    )(
        listed.reshape(-1).astype(jnp.int32),
        info,
        query_recv.reshape(rows, group_width),
        key_half.reshape(rows, group_width),
        key_other.reshape(rows, group_width),
        value_half.reshape(rows, group_width),
        value_other.reshape(rows, group_width),
    )
    returned = lax.all_to_all(
        attended.reshape(devices, block_len, group_width),
        "seq",
        split_axis=0,
        concat_axis=0,
        tiled=True,
    )
    returned = returned.reshape(documents, head_groups, 2, block_len, group_width).transpose(
        0, 2, 3, 1, 4
    )
    return returned.reshape(documents, 2 * block_len, head_groups * group_width)


def solution(mesh):
    placed = (
        P("groups", "seq", None),
        P("groups", "seq", None),
        P("groups", "seq", None),
        P("groups", None, None),
        P("groups", None),
    )

    def body(queries, *others):
        heads = queries.shape[2] // HEAD_DIM
        groups_needed = lax.axis_size("seq") // queries.shape[0]
        if heads % (groups_needed * CHUNK_HEADS) == 0:
            return per_device_fused(queries, *others)
        return per_device(queries, *others)

    return jax.shard_map(
        body, mesh=mesh, in_specs=placed, out_specs=P("groups", "seq", None), check_vma=False
    )
```
